32 devices in a mesh: src: 8 (over z, core), cand: 4 (over y, x).
Axes of the slice: x: 2, y: 2, z: 4, core: 2. Of those that a mesh axis runs over, the one named last changes fastest.
Arguments:
- layer_input: bfloat16 [32, 128, 1024], P(('src', 'cand')), parts along dimension 0, may hold values from -16 to 16
- token_ids: int32 [32, 128], P(('src', 'cand')), parts along dimension 0, may hold values from 0 to 50264
- lengths: int32 [32], P(('src', 'cand')), parts along dimension 0, may hold values from 32 to 128
- idf_table: float32 [402120], P('src'), parts along dimension 0, may hold values from 1 to 12
- query_weight: bfloat16 [1024, 1024], P('cand'), may hold values from -0.1875 to 0.1875
- key_weight: bfloat16 [1024, 1024], P('cand'), may hold values from -0.1875 to 0.1875
- value_weight: bfloat16 [1024, 1024], P('cand'), may hold values from -0.1875 to 0.1875
- output_weight: bfloat16 [1024, 1024], P('cand'), may hold values from -0.1875 to 0.1875
Outputs:
- embedded: bfloat16 [32, 128, 1024], P(('src', 'cand')), parts along dimension 0
- pair_utility: float32 [32, 4], P(('src', 'cand')), parts along dimension 0
- expected_utility: float32 [32], P(('src', 'cand')), parts along dimension 0
The draws below stay inside these ranges and needn't reach their ends.
There are 8 independent parts, one for each index of `src`. The reference program is written for one: setup_inputs(seed, part) draws one part's arguments, and reference() takes and returns one part's arrays. A program takes and returns all parts, laid end to end along the dimension named above; an argument that names none is the same for every part. Nothing has to cross between parts.
All inputs are finite; a program needn't handle non-finite values.
Results may differ from the reference program's by a relative error of at most 0.0086.
Values may be sent and summed in bfloat16 or wider, within the bound.
A program may use at most 64 MiB of HBM per device.

```python
import math
import jax
import jax.numpy as jnp
import numpy as np
from jax import lax

D = 1024
HEADS = 16
HEAD = 64
VOCAB = 50265
L = 128
CANDS = 4


def draw_layer_input(key, part):
    base = jax.random.normal(jax.random.fold_in(key, 21), (L, D), jnp.float32)
    noise = jax.random.normal(key, (CANDS, L, D), jnp.float32)
    mixing = jax.random.uniform(jax.random.fold_in(key, 22), (CANDS, 1, 1), jnp.float32, 0.3, 0.9)
    offsets = jax.random.randint(jax.random.fold_in(key, 23), (CANDS, 1), 0, 4)
    positions = jnp.arange(L, dtype=jnp.int32)[None, :]
    source_rows = (positions + offsets) % L
    replaced = jax.random.randint(jax.random.fold_in(key, 24), (CANDS, L), 0, 10) == 0
    other_rows = jax.random.randint(jax.random.fold_in(key, 25), (CANDS, L), 0, L)
    source_rows = jnp.where(replaced, other_rows, source_rows).astype(jnp.int32)
    shared_rows = jnp.take(base, source_rows.reshape(CANDS * L), axis=0).reshape(CANDS, L, D)
    values = mixing * shared_rows + jnp.sqrt(1.0 - mixing * mixing) * noise
    values = jnp.clip(values, -4.0, 4.0)
    return values.astype(jnp.bfloat16)


def place_ends(result, key, low, top_value):
    extent = result.shape
    spot = [jax.random.randint(jax.random.fold_in(key, axis), (), 0, extent[axis]) for axis in range(len(extent))]
    result = result.at[tuple(spot)].set(low)
    longest = extent.index(max(extent))
    spot[longest] = (spot[longest] + 1) % extent[longest]
    return result.at[tuple(spot)].set(top_value)


def level_of(key, shape, shards, least, largest):
    def one(axis_at, shards_of):
        draws = jax.random.uniform(jax.random.fold_in(jax.random.fold_in(key, 6), axis_at), (shards_of,), jnp.float32, least / len(shards), largest / len(shards))
        return jnp.repeat(jnp.exp(draws), shape[axis_at] // shards_of).reshape((-1,) + (1,) * (len(shape) - axis_at - 1))

    gain = one(*shards[0])
    for cut in shards[1:]:
        gain = gain * one(*cut)
    return gain


def cumulative_ranks(amount, skew):
    portions = [(1 << 20) // math.isqrt(rank ** skew) + 1 for rank in range(1, amount + 1)]
    scale = 1 + sum(portions) // (1 << 30)
    return np.cumsum(np.array([max(1, weight // scale) for weight in portions]))


def ranked_ids(key, extent, count, skew):
    listing = cumulative_ranks(count, skew)
    lot = jax.random.randint(jax.random.fold_in(key, 1), extent, 0, int(listing[count - 1]))
    rank = jnp.searchsorted(jnp.asarray(listing, jnp.int32), lot, side="right")
    return jax.random.permutation(jax.random.fold_in(key, 2), count)[rank].astype(jnp.int32)


def gaussian(stream_key, extent, width, bound, shards=(), held_as=jnp.bfloat16):
    factor_of = level_of(stream_key, extent, shards, -0.22, 0.18) if shards else 1.0
    array = jax.random.normal(stream_key, extent, jnp.float32) * width * factor_of
    return jnp.minimum(jnp.maximum(array, -bound), bound).astype(held_as)


def setup_inputs(seed: int = 0, part: int = 0) -> dict:
    keys = jax.random.split(jax.random.key(seed), 9)
    part_keys = jax.random.split(jax.random.fold_in(keys[8], part), 9)
    return {
        "layer_input": draw_layer_input(jax.random.fold_in(jax.random.fold_in(keys[8], part), 71), part),
        "token_ids": place_ends(ranked_ids(part_keys[1], (CANDS, L), VOCAB, 2), jax.random.fold_in(part_keys[1], 3), 0, VOCAB - 1).astype(jnp.int32),
        "lengths": place_ends(jax.random.randint(part_keys[2], (CANDS,), L // 4, L + 1), jax.random.fold_in(part_keys[2], 1), L // 4, L).astype(jnp.int32),
        "idf_table": jnp.clip(jnp.exp(jax.random.uniform(part_keys[3], (VOCAB,), jnp.float32, math.log(1.0), math.log(12.0))), 1.0, 12.0),
        "query_weight": gaussian(keys[4], (D, D), D ** -0.5, 0.1875, ((0, 4),)),
        "key_weight": gaussian(keys[5], (D, D), D ** -0.5, 0.1875, ((0, 4),)),
        "value_weight": gaussian(keys[6], (D, D), D ** -0.5, 0.1875, ((0, 4),)),
        "output_weight": gaussian(keys[7], (D, D), D ** -0.5, 0.1875, ((0, 4),)),
    }


def encode(layer_input, lengths, query_weight, key_weight, value_weight, output_weight):
    flat = layer_input.reshape(CANDS * L, D)

    def project(weight):
        return jnp.dot(flat, weight, preferred_element_type=jnp.float32).astype(jnp.bfloat16)
    queries = project(query_weight).reshape(CANDS, L, HEADS, HEAD)
    key_rows = project(key_weight).reshape(CANDS, L, HEADS, HEAD)
    value_rows = project(value_weight).reshape(CANDS, L, HEADS, HEAD)
    positions = jnp.arange(L, dtype=jnp.int32)
    valid = positions[None, :] < lengths[:, None]
    scale = 1.0 / math.sqrt(HEAD)
    scores = jnp.einsum('clhe,cmhe->chlm', queries.astype(jnp.float32), key_rows.astype(jnp.float32), precision=lax.Precision.HIGHEST) * scale
    scores = jnp.where(valid[:, None, None, :], scores, -1000000000.0)
    highest = lax.optimization_barrier(jnp.max(scores, axis=-1, keepdims=True))
    expo = jnp.exp(scores - highest)
    probs = (expo / lax.optimization_barrier(jnp.sum(expo, axis=-1, keepdims=True))).astype(jnp.bfloat16)
    context = jnp.einsum('chlm,cmhe->clhe', probs.astype(jnp.float32), value_rows.astype(jnp.float32), precision=lax.Precision.HIGHEST).astype(jnp.bfloat16).reshape(CANDS * L, D)
    mixed = jnp.dot(context, output_weight, preferred_element_type=jnp.float32) + flat.astype(jnp.float32)
    centred = mixed - lax.optimization_barrier(jnp.mean(mixed, axis=-1, keepdims=True))
    squares = lax.optimization_barrier(jnp.sum(centred * centred, axis=-1, keepdims=True))
    embedded = (centred / jnp.sqrt(squares + 0.001)).astype(jnp.bfloat16)
    return (embedded.reshape(CANDS, L, D), valid)

def reference(layer_input, token_ids, lengths, idf_table, query_weight, key_weight, value_weight, output_weight):
    embedded, valid = encode(layer_input, lengths, query_weight, key_weight, value_weight, output_weight)
    token_weight = (jnp.take(idf_table, token_ids, axis=0) * valid.astype(jnp.float32)).astype(jnp.bfloat16)
    flat_vectors = embedded.reshape(CANDS * L, D).astype(jnp.float32)
    similarity = jnp.dot(flat_vectors, flat_vectors.T, precision=lax.Precision.HIGHEST).reshape(CANDS, L, CANDS, L)
    usable = token_weight > 0
    best_other = lax.optimization_barrier(jnp.max(jnp.where(usable[None, None, :, :], similarity, -4.0), axis=3))
    weight_float = token_weight.astype(jnp.float32)
    forward = jnp.einsum('il,ilj->ij', weight_float, best_other, precision=lax.Precision.HIGHEST)
    forward = forward / lax.optimization_barrier(jnp.sum(weight_float, axis=1))[:, None]
    pair_utility = 0.5 * (forward + forward.T)
    diagonal = jnp.diagonal(pair_utility)
    expected_utility = (lax.optimization_barrier(jnp.sum(pair_utility, axis=1)) - diagonal) / (CANDS - 1)
    return (embedded, pair_utility, expected_utility)
```

```python
import functools
import math

import jax
import jax.numpy as jnp
from jax import lax
from jax.experimental import pallas as pl
from jax.experimental.pallas import tpu as pltpu
from jax.sharding import PartitionSpec as P

HEAD = 64


def block_utility(own_vectors, own_weight, far_vectors, far_weight):
    own_count, length, width = own_vectors.shape
    far_count = far_vectors.shape[0]
    similar = lax.dot_general(
        own_vectors.reshape(own_count * length, width),
        far_vectors.reshape(far_count * length, width),
        (((1,), (1,)), ((), ())),
        preferred_element_type=jnp.float32,
    )
    similar = similar.reshape(own_count, length, far_count, length)
    own_usable = own_weight > 0
    far_usable = far_weight > 0
    best_far = jnp.max(jnp.where(far_usable[None, None, :, :], similar, -4.0), axis=3)
    best_own = jnp.max(jnp.where(own_usable[:, :, None, None], similar, -4.0), axis=1)
    own_float = own_weight.astype(jnp.float32)
    far_float = far_weight.astype(jnp.float32)
    forward = jnp.einsum("il,ilj->ij", own_float, best_far, precision=lax.Precision.HIGHEST)
    forward = forward / jnp.sum(own_float, axis=1)[:, None]
    backward = jnp.einsum("jm,ijm->ij", far_float, best_own, precision=lax.Precision.HIGHEST)
    backward = backward / jnp.sum(far_float, axis=1)[None, :]
    return 0.5 * (forward + backward)


def gathered_shards(
    layer_input,
    token_ids,
    lengths,
    idf_table,
    query_weight,
    key_weight,
    value_weight,
    output_weight,
):
    local_cands, length, width = layer_input.shape
    cycle_size = lax.axis_size("cand")
    all_cands = local_cands * cycle_size
    head_size = HEAD
    head_count = width // head_size
    flat = layer_input.reshape(local_cands * length, width)
    pieces = (
        lax.all_gather(query_weight, "cand", axis=0, tiled=True),
        lax.all_gather(key_weight, "cand", axis=0, tiled=True),
        lax.all_gather(value_weight, "cand", axis=0, tiled=True),
    )
    columns = flat
    queries, key_rows, value_rows = tuple(
        (jnp.dot(columns, piece, preferred_element_type=jnp.float32) for piece in pieces)
    )
    queries = queries.astype(jnp.bfloat16).reshape(local_cands, length, head_count, head_size)
    key_rows = key_rows.astype(jnp.bfloat16).reshape(local_cands, length, head_count, head_size)
    value_rows = value_rows.astype(jnp.bfloat16).reshape(local_cands, length, head_count, head_size)
    positions = jnp.arange(length, dtype=jnp.int32)
    valid = positions[None, :] < lengths[:, None]
    scale = 1.0 / math.sqrt(head_size)
    scores = (
        jnp.einsum("clhe,cmhe->chlm", queries, key_rows, preferred_element_type=jnp.float32) * scale
    )
    scores = jnp.where(valid[:, None, None, :], scores, -1000000000.0)
    highest = jnp.max(scores, axis=-1, keepdims=True)
    expo = jnp.exp(scores - highest)
    probs = (expo / jnp.sum(expo, axis=-1, keepdims=True)).astype(jnp.bfloat16)
    context = jnp.einsum("chlm,cmhe->clhe", probs, value_rows, preferred_element_type=jnp.float32)
    context = context.astype(jnp.bfloat16).reshape(local_cands * length, width)
    columns = context
    mixed = jnp.dot(
        columns,
        lax.all_gather(output_weight, "cand", axis=0, tiled=True),
        preferred_element_type=jnp.float32,
    ) + flat.astype(jnp.float32)
    centred = mixed - jnp.mean(mixed, axis=-1, keepdims=True)
    squares = jnp.sum(centred * centred, axis=-1, keepdims=True)
    embedded = (
        (centred / jnp.sqrt(squares + 0.001))
        .astype(jnp.bfloat16)
        .reshape(local_cands, length, width)
    )
    token_weight = (jnp.take(idf_table, token_ids, axis=0) * valid.astype(jnp.float32)).astype(
        jnp.bfloat16
    )
    myself = lax.axis_index("cand")
    piece = (
        lax.all_gather(embedded, "cand", axis=0, tiled=True),
        lax.all_gather(token_weight, "cand", axis=0, tiled=True),
    )
    utility = block_utility(embedded, token_weight, piece[0], piece[1])
    blocks = utility.reshape(local_cands, cycle_size, local_cands)
    own_part = lax.dynamic_slice(blocks, (0, myself, 0), (local_cands, 1, local_cands))[:, 0, :]
    diagonal = jnp.diagonal(own_part)
    expected_utility = (jnp.sum(utility, axis=1) - diagonal) / (all_cands - 1)
    return (embedded, utility, expected_utility)


def remote(src_ref, dst_ref, send_sem, recv_sem, device):
    return pltpu.make_async_remote_copy(
        src_ref=src_ref,
        dst_ref=dst_ref,
        send_sem=send_sem,
        recv_sem=recv_sem,
        device_id=device,
        device_id_type=pl.DeviceIdType.MESH,
    )


def flipped(index, bits):
    result = index
    place = 1
    while place <= bits:
        if bits & place:
            digit = lax.rem(lax.div(index, place), 2)
            result = result + place - 2 * place * digit
        place *= 2
    return result


def kernel(
    count,
    x_hbm,
    meta_hbm,
    q_hbm,
    k_hbm,
    v_hbm,
    o_hbm,
    embedded_hbm,
    utility_ref,
    expected_ref,
    stage,
    full,
    out_rows,
    x_all,
    meta,
    part_out,
    part_in,
    vectors,
    local_sem,
    w_send,
    w_recv,
    f_send,
    f_recv,
    x_send,
    x_recv,
    m_send,
    m_recv,
    p_send,
    p_recv,
    e_send,
    e_recv,
):
    group, me = lax.axis_index("src"), lax.axis_index("cand")
    core = lax.rem(group, 2)
    sibling = (flipped(group, 1), me)
    others = range(1, count)
    peer = [(group, flipped(me, bits)) for bits in range(count)]
    length, width = x_hbm.shape
    rows, columns = stage.shape[1], full.shape[2]
    half = rows // 2

    def column_block(index):
        return pl.ds(pl.multiple_of(index * columns, columns), columns)

    def row_block(index):
        return pl.ds(pl.multiple_of(index * rows, rows), rows)

    def row_half(index, which):
        return pl.ds(pl.multiple_of(index * rows + which * half, half), half)

    own_half = pl.ds(pl.multiple_of(core * half, half), half)

    weights = (q_hbm, k_hbm, v_hbm)
    loads = [pltpu.make_async_copy(w, stage.at[t], local_sem.at[t]) for t, w in enumerate(weights)]
    loads += [
        pltpu.make_async_copy(x_hbm, x_all.at[0], local_sem.at[3]),
        pltpu.make_async_copy(meta_hbm, meta.at[0], local_sem.at[4]),
    ]
    loads += [
        pltpu.make_async_copy(
            w.at[:, column_block(me)], full.at[t, row_block(me), :], local_sem.at[5 + t]
        )
        for t, w in enumerate(weights)
    ]
    loads += [pltpu.make_async_copy(o_hbm, out_rows, local_sem.at[8])]
    for load in loads:
        load.start()

    barrier = pltpu.get_barrier_semaphore()
    for target in [sibling] + [peer[r] for r in others]:
        pl.semaphore_signal(barrier, inc=1, device_id=target, device_id_type=pl.DeviceIdType.MESH)
    pl.semaphore_wait(barrier, count)

    for t in range(3):
        loads[t].wait()
    w_copies, f_copies, x_copies, m_copies = {}, {}, {}, {}
    for r in others:
        w_copies[r] = remote(
            stage.at[:, own_half, column_block(peer[r][1])],
            full.at[:, row_half(me, core), :],
            w_send.at[r],
            w_recv.at[r],
            peer[r],
        )
        w_copies[r].start()
    loads[3].wait()
    loads[4].wait()
    for r in others:
        m_copies[r] = remote(meta.at[0], meta.at[r], m_send.at[r], m_recv.at[r], peer[r])
        m_copies[r].start()
    for r in others:
        x_copies[r] = remote(x_all.at[0], x_all.at[r], x_send.at[r], x_recv.at[r], peer[r])
        x_copies[r].start()
    for r in others:
        w_copies[r].wait_recv()
        landed = full.at[:, row_half(peer[r][1], core), :]
        f_copies[r] = remote(landed, landed, f_send.at[r], f_recv.at[r], sibling)
        f_copies[r].start()
    for load in loads[5:]:
        load.wait()
    for r in others:
        f_copies[r].wait_recv()

    lane = lax.broadcasted_iota(jnp.int32, (1, 2 * HEAD), 1)
    scale = 1.0 / math.sqrt(HEAD)
    first = (lane < HEAD).astype(jnp.float32)
    keep = [(first * scale).astype(jnp.bfloat16), ((1.0 - first) * scale).astype(jnp.bfloat16)]

    def partial_of(r):
        rows_in = x_all[r]
        queries, key_rows, value_rows = tuple(
            jnp.dot(rows_in, full[t], preferred_element_type=jnp.float32).astype(jnp.bfloat16)
            for t in range(3)
        )
        valid = meta[r, 1:2, :] > 0.0
        pieces = []
        for start in range(0, columns, 2 * HEAD):
            span = slice(start, start + 2 * HEAD)
            q_pair, k_pair, v_pair = queries[:, span], key_rows[:, span], value_rows[:, span]
            stacked = jnp.concatenate([q_pair * keep[0], q_pair * keep[1]], axis=0)
            scores = lax.dot_general(
                stacked, k_pair, (((1,), (1,)), ((), ())), preferred_element_type=jnp.float32
            )
            scores = jnp.where(valid, scores, -1000000000.0)
            expo = jnp.exp(scores - jnp.max(scores, axis=-1, keepdims=True))
            total = jnp.sum(expo, axis=-1, keepdims=True)
            summed = jnp.dot(
                expo.astype(jnp.bfloat16), v_pair, preferred_element_type=jnp.float32
            )
            summed = summed / total
            pieces.append(jnp.where(lane < HEAD, summed[:length], summed[length:]))
        context = jnp.concatenate(pieces, axis=1).astype(jnp.bfloat16)
        return jnp.dot(context, out_rows[...], preferred_element_type=jnp.float32)

    mixed = partial_of(0) + x_all[0].astype(jnp.float32)
    p_copies = {}
    for r in others:
        x_copies[r].wait_recv()
        m_copies[r].wait_recv()
        part_out[r] = partial_of(r).astype(jnp.bfloat16)
        p_copies[r] = remote(part_out.at[r], part_in.at[r], p_send.at[r], p_recv.at[r], peer[r])
        p_copies[r].start()
    for r in others:
        p_copies[r].wait_recv()
        mixed = mixed + part_in[r].astype(jnp.float32)
    centred = mixed - jnp.mean(mixed, axis=-1, keepdims=True)
    squares = jnp.sum(centred * centred, axis=-1, keepdims=True)
    own = (centred / jnp.sqrt(squares + 0.001)).astype(jnp.bfloat16)
    vectors[0] = own
    e_copies = {}
    for r in others:
        e_copies[r] = remote(vectors.at[0], vectors.at[r], e_send.at[r], e_recv.at[r], peer[r])
        e_copies[r].start()
    store = pltpu.make_async_copy(vectors.at[0], embedded_hbm, local_sem.at[0])
    store.start()

    own_weight = meta[0, 0:1, :]
    own_column = jnp.broadcast_to(own_weight, (length, length)).T
    own_total = jnp.sum(own_weight, axis=1, keepdims=True)
    slot = lax.broadcasted_iota(jnp.int32, utility_ref.shape, 1)
    utility = jnp.zeros(utility_ref.shape, jnp.float32)
    everything = jnp.zeros((1, 1), jnp.float32)
    diagonal = None
    for r in range(count):
        if r:
            e_copies[r].wait_recv()
        far_weight = meta[r, 0:1, :]
        similar = lax.dot_general(
            own, vectors[r], (((1,), (1,)), ((), ())), preferred_element_type=jnp.float32
        )
        best_far = jnp.max(jnp.where(far_weight > 0, similar, -4.0), axis=1, keepdims=True)
        best_own = jnp.max(jnp.where(own_column > 0, similar, -4.0), axis=0, keepdims=True)
        forward = jnp.sum(own_column[:, 0:1] * best_far, axis=0, keepdims=True) / own_total
        backward = jnp.sum(far_weight * best_own, axis=1, keepdims=True) / jnp.sum(
            far_weight, axis=1, keepdims=True
        )
        pair = 0.5 * (forward + backward)
        utility = jnp.where(slot == peer[r][1], pair, utility)
        everything = everything + pair
        if r == 0:
            diagonal = pair
    utility_ref[...] = utility
    expected_ref[...] = (everything - diagonal) / (count - 1)

    store.wait()
    for r in others:
        for copies in (w_copies, f_copies, x_copies, m_copies, p_copies, e_copies):
            copies[r].wait_send()


def shards(
    sizes,
    layer_input,
    token_ids,
    lengths,
    idf_table,
    query_weight,
    key_weight,
    value_weight,
    output_weight,
):
    local_cands, length, width = layer_input.shape
    count = sizes["cand"]
    rows = query_weight.shape[0]
    columns = width // count
    if (
        local_cands != 1
        or count < 2
        or count & (count - 1)
        or sizes["src"] % 2
        or columns % (2 * HEAD)
        or rows % 32
        or length != 128
    ):
        return gathered_shards(
            layer_input,
            token_ids,
            lengths,
            idf_table,
            query_weight,
            key_weight,
            value_weight,
            output_weight,
        )
    valid = (jnp.arange(length, dtype=jnp.int32)[None, :] < lengths[:, None]).astype(jnp.float32)
    token_weight = jnp.take(idf_table, token_ids, axis=0) * valid
    token_weight = token_weight.astype(jnp.bfloat16).astype(jnp.float32)
    row = lax.broadcasted_iota(jnp.int32, (8, length), 0)
    meta = jnp.where(row == 0, token_weight, valid)
    anywhere = pl.BlockSpec(memory_space=pl.ANY)
    in_vmem = pl.BlockSpec(memory_space=pltpu.VMEM)
    pairs = pltpu.SemaphoreType.DMA((count,))
    embedded, utility, expected = pl.pallas_call(
        functools.partial(kernel, count),
        out_shape=(
            jax.ShapeDtypeStruct((length, width), jnp.bfloat16),
            jax.ShapeDtypeStruct((1, count), jnp.float32),
            jax.ShapeDtypeStruct((1, 1), jnp.float32),
        ),
        in_specs=[anywhere] * 6,
        out_specs=(anywhere, in_vmem, in_vmem),
        scratch_shapes=[
            pltpu.VMEM((3, rows, width), jnp.bfloat16),
            pltpu.VMEM((3, rows * count, columns), jnp.bfloat16),
            pltpu.VMEM((rows, width), jnp.bfloat16),
            pltpu.VMEM((count, length, width), jnp.bfloat16),
            pltpu.VMEM((count, 8, length), jnp.float32),
            pltpu.VMEM((count, length, width), jnp.bfloat16),
            pltpu.VMEM((count, length, width), jnp.bfloat16),
            pltpu.VMEM((count, length, width), jnp.bfloat16),
            pltpu.SemaphoreType.DMA((9,)),
        ]
        + [pairs] * 12,
        compiler_params=pltpu.CompilerParams(collective_id=0, has_side_effects=True),
    )(
        layer_input.reshape(length, width),
        meta,
        query_weight,
        key_weight,
        value_weight,
        output_weight,
    )
    return (embedded.reshape(1, length, width), utility, expected.reshape(1))


def solution(mesh):
    in_specs = (
        P(("src", "cand"), None, None),
        P(("src", "cand"), None),
        P(("src", "cand")),
        P("src"),
        P("cand", None),
        P("cand", None),
        P("cand", None),
        P("cand", None),
    )
    out_specs = (P(("src", "cand"), None, None), P(("src", "cand"), None), P(("src", "cand")))
    return jax.shard_map(
        functools.partial(shards, dict(mesh.shape)),
        mesh=mesh,
        in_specs=in_specs,
        out_specs=out_specs,
        check_vma=False,
    )
```

```python
import functools
import math

import jax
import jax.numpy as jnp
from jax import lax
from jax.experimental import pallas as pl
from jax.experimental.pallas import tpu as pltpu
from jax.sharding import PartitionSpec as P

HEAD = 64


def block_utility(own_vectors, own_weight, far_vectors, far_weight):
    own_count, length, width = own_vectors.shape
    far_count = far_vectors.shape[0]
    similar = lax.dot_general(
        own_vectors.reshape(own_count * length, width),
        far_vectors.reshape(far_count * length, width),
        (((1,), (1,)), ((), ())),
        preferred_element_type=jnp.float32,
    )
    similar = similar.reshape(own_count, length, far_count, length)
    own_usable = own_weight > 0
    far_usable = far_weight > 0
    best_far = jnp.max(jnp.where(far_usable[None, None, :, :], similar, -4.0), axis=3)
    best_own = jnp.max(jnp.where(own_usable[:, :, None, None], similar, -4.0), axis=1)
    own_float = own_weight.astype(jnp.float32)
    far_float = far_weight.astype(jnp.float32)
    forward = jnp.einsum("il,ilj->ij", own_float, best_far, precision=lax.Precision.HIGHEST)
    forward = forward / jnp.sum(own_float, axis=1)[:, None]
    backward = jnp.einsum("jm,ijm->ij", far_float, best_own, precision=lax.Precision.HIGHEST)
    backward = backward / jnp.sum(far_float, axis=1)[None, :]
    return 0.5 * (forward + backward)


def gathered_shards(
    layer_input,
    token_ids,
    lengths,
    idf_table,
    query_weight,
    key_weight,
    value_weight,
    output_weight,
):
    local_cands, length, width = layer_input.shape
    cycle_size = lax.axis_size("cand")
    all_cands = local_cands * cycle_size
    head_size = HEAD
    head_count = width // head_size
    flat = layer_input.reshape(local_cands * length, width)
    pieces = (
        lax.all_gather(query_weight, "cand", axis=0, tiled=True),
        lax.all_gather(key_weight, "cand", axis=0, tiled=True),
        lax.all_gather(value_weight, "cand", axis=0, tiled=True),
    )
    columns = flat
    queries, key_rows, value_rows = tuple(
        (jnp.dot(columns, piece, preferred_element_type=jnp.float32) for piece in pieces)
    )
    queries = queries.astype(jnp.bfloat16).reshape(local_cands, length, head_count, head_size)
    key_rows = key_rows.astype(jnp.bfloat16).reshape(local_cands, length, head_count, head_size)
    value_rows = value_rows.astype(jnp.bfloat16).reshape(local_cands, length, head_count, head_size)
    positions = jnp.arange(length, dtype=jnp.int32)
    valid = positions[None, :] < lengths[:, None]
    scale = 1.0 / math.sqrt(head_size)
    scores = (
        jnp.einsum("clhe,cmhe->chlm", queries, key_rows, preferred_element_type=jnp.float32) * scale
    )
    scores = jnp.where(valid[:, None, None, :], scores, -1000000000.0)
    highest = jnp.max(scores, axis=-1, keepdims=True)
    expo = jnp.exp(scores - highest)
    probs = (expo / jnp.sum(expo, axis=-1, keepdims=True)).astype(jnp.bfloat16)
    context = jnp.einsum("chlm,cmhe->clhe", probs, value_rows, preferred_element_type=jnp.float32)
    context = context.astype(jnp.bfloat16).reshape(local_cands * length, width)
    columns = context
    mixed = jnp.dot(
        columns,
        lax.all_gather(output_weight, "cand", axis=0, tiled=True),
        preferred_element_type=jnp.float32,
    ) + flat.astype(jnp.float32)
    centred = mixed - jnp.mean(mixed, axis=-1, keepdims=True)
    squares = jnp.sum(centred * centred, axis=-1, keepdims=True)
    embedded = (
        (centred / jnp.sqrt(squares + 0.001))
        .astype(jnp.bfloat16)
        .reshape(local_cands, length, width)
    )
    token_weight = (jnp.take(idf_table, token_ids, axis=0) * valid.astype(jnp.float32)).astype(
        jnp.bfloat16
    )
    myself = lax.axis_index("cand")
    piece = (
        lax.all_gather(embedded, "cand", axis=0, tiled=True),
        lax.all_gather(token_weight, "cand", axis=0, tiled=True),
    )
    utility = block_utility(embedded, token_weight, piece[0], piece[1])
    blocks = utility.reshape(local_cands, cycle_size, local_cands)
    own_part = lax.dynamic_slice(blocks, (0, myself, 0), (local_cands, 1, local_cands))[:, 0, :]
    diagonal = jnp.diagonal(own_part)
    expected_utility = (jnp.sum(utility, axis=1) - diagonal) / (all_cands - 1)
    return (embedded, utility, expected_utility)


def remote(src_ref, dst_ref, send_sem, recv_sem, device):
    return pltpu.make_async_remote_copy(
        src_ref=src_ref,
        dst_ref=dst_ref,
        send_sem=send_sem,
        recv_sem=recv_sem,
        device_id=device,
        device_id_type=pl.DeviceIdType.MESH,
    )


def flipped(index, bits):
    result = index
    place = 1
    while place <= bits:
        if bits & place:
            digit = lax.rem(lax.div(index, place), 2)
            result = result + place - 2 * place * digit
        place *= 2
    return result


def kernel(
    count,
    x_hbm,
    meta_hbm,
    q_hbm,
    k_hbm,
    v_hbm,
    o_hbm,
    embedded_ref,
    utility_ref,
    expected_ref,
    stage,
    full,
    out_full,
    x_all,
    meta,
    context_out,
    context_full,
    vectors,
    local_sem,
    send_sem,
    recv_sem,
):
    group, me = lax.axis_index("src"), lax.axis_index("cand")
    share = lax.rem(group, 4)
    sibling = (flipped(group, 1), me)
    mate = (flipped(group, 2), me)
    others = range(1, count)
    peer = [(group, flipped(me, bits)) for bits in range(count)]
    length, width = x_hbm.shape
    rows, columns = stage.shape[1], full.shape[2]
    quarter, middle = rows // 4, length // 2
    started = []

    def push(src_ref, dst_ref, device):
        number = len(started)
        copy = remote(src_ref, dst_ref, send_sem.at[number], recv_sem.at[number], device)
        copy.start()
        started.append(copy)
        return copy

    def column_block(index):
        return pl.ds(pl.multiple_of(index * columns, columns), columns)

    def row_block(index):
        return pl.ds(pl.multiple_of(index * rows, rows), rows)

    def row_share(index, which):
        return pl.ds(pl.multiple_of(index * rows + which * quarter, quarter), quarter)

    own_share = pl.ds(pl.multiple_of(share * quarter, quarter), quarter)
    mate_share = lax.rem(share + 2, 4)

    weights = (q_hbm, k_hbm, v_hbm)
    loads = [pltpu.make_async_copy(w, stage.at[t], local_sem.at[t]) for t, w in enumerate(weights)]
    loads += [
        pltpu.make_async_copy(o_hbm, out_full.at[row_block(me), :], local_sem.at[3]),
        pltpu.make_async_copy(x_hbm, x_all.at[0], local_sem.at[4]),
        pltpu.make_async_copy(meta_hbm, meta.at[0], local_sem.at[5]),
    ]
    loads += [
        pltpu.make_async_copy(
            w.at[:, column_block(me)], full.at[t, row_block(me), :], local_sem.at[6 + t]
        )
        for t, w in enumerate(weights)
    ]
    for load in loads:
        load.start()

    barrier = pltpu.get_barrier_semaphore()
    targets = [sibling, mate] + [peer[r] for r in others]
    for target in targets:
        pl.semaphore_signal(barrier, inc=1, device_id=target, device_id_type=pl.DeviceIdType.MESH)
    pl.semaphore_wait(barrier, len(targets))

    def exchange(held):
        part = [held.at[0, pl.ds(0, middle), :], held.at[0, pl.ds(middle, middle), :]]

        def slot(r, which):
            return held.at[r, pl.ds(which * middle, middle), :]

        first = {1: push(part[0], slot(1, 0), peer[1]), 2: push(part[1], slot(2, 1), peer[2])}
        second = {1: push(part[1], slot(1, 1), peer[1]), 2: push(part[0], slot(2, 0), peer[2])}

        def relay():
            first[1].wait_recv()
            near = push(slot(1, 0), slot(3, 0), peer[2])
            first[2].wait_recv()
            return (near, push(slot(2, 1), slot(3, 1), peer[1]))

        return second, relay

    for t in range(3):
        loads[t].wait()
    w_copies = {}
    for r in others:
        w_copies[r] = push(
            stage.at[:, own_share, column_block(peer[r][1])],
            full.at[:, row_share(me, share), :],
            peer[r],
        )
    for load in loads[3:6]:
        load.wait()
    m_copies = {r: push(meta.at[0], meta.at[r], peer[r]) for r in others}
    o_copies = {
        r: push(out_full.at[row_share(me, share), :], out_full.at[row_share(me, share), :], peer[r])
        for r in others
    }
    x_second, x_relay = exchange(x_all)
    for load in loads[6:]:
        load.wait()

    def spread(copy, landed):
        copy.wait_recv()
        return (push(landed, landed, mate), push(landed, landed, sibling))

    def hand_over(copy, landed):
        copy.wait_recv()
        return push(landed, landed, sibling)

    def full_share(r, which):
        return full.at[:, row_share(peer[r][1], which), :]

    def out_share(r, which):
        return out_full.at[row_share(peer[r][1], which), :]

    w_spread = {r: spread(w_copies[r], full_share(r, share)) for r in others}
    o_spread = {}
    o_hand = {}
    for r in others:
        o_spread[r] = spread(o_copies[r], out_share(r, share))
    w_hand = {r: hand_over(w_spread[r][0], full_share(r, mate_share)) for r in others}
    x_far = x_relay()
    for r in others:
        w_spread[r][1].wait_recv()
        w_hand[r].wait_recv()

    lane = lax.broadcasted_iota(jnp.int32, (1, 2 * HEAD), 1)
    scale = 1.0 / math.sqrt(HEAD)
    first = (lane < HEAD).astype(jnp.float32)
    keep = [(first * scale).astype(jnp.bfloat16), ((1.0 - first) * scale).astype(jnp.bfloat16)]

    def context_of(r):
        rows_in = x_all[r]
        queries, key_rows, value_rows = tuple(
            jnp.dot(rows_in, full[t], preferred_element_type=jnp.float32).astype(jnp.bfloat16)
            for t in range(3)
        )
        valid = meta[r, 1:2, :] > 0.0
        pieces = []
        for start in range(0, columns, 2 * HEAD):
            span = slice(start, start + 2 * HEAD)
            q_pair, k_pair, v_pair = queries[:, span], key_rows[:, span], value_rows[:, span]
            stacked = jnp.concatenate([q_pair * keep[0], q_pair * keep[1]], axis=0)
            scores = lax.dot_general(
                stacked, k_pair, (((1,), (1,)), ((), ())), preferred_element_type=jnp.float32
            )
            scores = jnp.where(valid, scores, -1000000000.0)
            expo = jnp.exp(scores - jnp.max(scores, axis=-1, keepdims=True))
            total = jnp.sum(expo, axis=-1, keepdims=True)
            summed = jnp.dot(
                expo.astype(jnp.bfloat16), v_pair, preferred_element_type=jnp.float32
            )
            summed = summed / total
            pieces.append(jnp.where(lane < HEAD, summed[:length], summed[length:]))
        return jnp.concatenate(pieces, axis=1).astype(jnp.bfloat16)

    context_full[:, column_block(me)] = context_of(0)
    c_copies = []
    for r in others:
        m_copies[r].wait_recv()
        for copy in ((x_second[r],) if r < 3 else x_far):
            copy.wait_recv()
        context_out[r] = context_of(r)
        c_copies.append(push(context_out.at[r], context_full.at[:, column_block(me)], peer[r]))
        if r == 2:
            for q in others:
                o_hand[q] = hand_over(o_spread[q][0], out_share(q, mate_share))
    for r in others:
        o_spread[r][1].wait_recv()
        o_hand[r].wait_recv()
    for copy in c_copies:
        copy.wait_recv()

    mixed = jnp.dot(context_full[...], out_full[...], preferred_element_type=jnp.float32)
    mixed = mixed + x_all[0].astype(jnp.float32)
    centred = mixed - jnp.mean(mixed, axis=-1, keepdims=True)
    squares = jnp.sum(centred * centred, axis=-1, keepdims=True)
    own = (centred / jnp.sqrt(squares + 0.001)).astype(jnp.bfloat16)
    vectors[0] = own
    e_second, e_relay = exchange(vectors)
    store = pltpu.make_async_copy(vectors.at[0], embedded_ref, local_sem.at[0])
    store.start()

    own_weight = meta[0, 0:1, :]
    own_column = jnp.broadcast_to(own_weight, (length, length)).T
    own_total = jnp.sum(own_weight, axis=1, keepdims=True)
    slot = lax.broadcasted_iota(jnp.int32, utility_ref.shape, 1)

    def pair_of(r):
        far_weight = meta[r, 0:1, :]
        similar = lax.dot_general(
            own, vectors[r], (((1,), (1,)), ((), ())), preferred_element_type=jnp.float32
        )
        best_far = jnp.max(jnp.where(far_weight > 0, similar, -4.0), axis=1, keepdims=True)
        best_own = jnp.max(jnp.where(own_column > 0, similar, -4.0), axis=0, keepdims=True)
        forward = jnp.sum(own_column[:, 0:1] * best_far, axis=0, keepdims=True) / own_total
        backward = jnp.sum(far_weight * best_own, axis=1, keepdims=True) / jnp.sum(
            far_weight, axis=1, keepdims=True
        )
        return 0.5 * (forward + backward)

    diagonal = pair_of(0)
    e_far = e_relay()
    utility = jnp.where(slot == me, diagonal, 0.0)
    everything = diagonal
    for r in others:
        for copy in ((e_second[r],) if r < 3 else e_far):
            copy.wait_recv()
        pair = pair_of(r)
        utility = jnp.where(slot == peer[r][1], pair, utility)
        everything = everything + pair
    utility_ref[...] = utility
    expected_ref[...] = (everything - diagonal) / (count - 1)

    for copy in started:
        copy.wait_send()
    store.wait()


def shards(
    sizes,
    layer_input,
    token_ids,
    lengths,
    idf_table,
    query_weight,
    key_weight,
    value_weight,
    output_weight,
):
    local_cands, length, width = layer_input.shape
    count = sizes["cand"]
    rows = query_weight.shape[0]
    columns = width // count
    if (
        local_cands != 1
        or count != 4
        or sizes["src"] % 4
        or columns % (2 * HEAD)
        or rows % 64
        or length != 128
    ):
        return gathered_shards(
            layer_input,
            token_ids,
            lengths,
            idf_table,
            query_weight,
            key_weight,
            value_weight,
            output_weight,
        )
    valid = (jnp.arange(length, dtype=jnp.int32)[None, :] < lengths[:, None]).astype(jnp.float32)
    token_weight = jnp.take(idf_table, token_ids, axis=0) * valid
    token_weight = token_weight.astype(jnp.bfloat16).astype(jnp.float32)
    row = lax.broadcasted_iota(jnp.int32, (8, length), 0)
    meta = jnp.where(row == 0, token_weight, valid)
    anywhere = pl.BlockSpec(memory_space=pl.ANY)
    in_vmem = pl.BlockSpec(memory_space=pltpu.VMEM)
    copies = pltpu.SemaphoreType.DMA((42,))
    embedded, utility, expected = pl.pallas_call(
        functools.partial(kernel, count),
        out_shape=(
            jax.ShapeDtypeStruct((length, width), jnp.bfloat16),
            jax.ShapeDtypeStruct((1, count), jnp.float32),
            jax.ShapeDtypeStruct((1, 1), jnp.float32),
        ),
        in_specs=[anywhere] * 6,
        out_specs=(anywhere, in_vmem, in_vmem),
        scratch_shapes=[
            pltpu.VMEM((3, rows, width), jnp.bfloat16),
            pltpu.VMEM((3, rows * count, columns), jnp.bfloat16),
            pltpu.VMEM((rows * count, width), jnp.bfloat16),
            pltpu.VMEM((count, length, width), jnp.bfloat16),
            pltpu.VMEM((count, 8, length), jnp.float32),
            pltpu.VMEM((count, length, columns), jnp.bfloat16),
            pltpu.VMEM((length, width), jnp.bfloat16),
            pltpu.VMEM((count, length, width), jnp.bfloat16),
            pltpu.SemaphoreType.DMA((9,)),
            copies,
            copies,
        ],
        compiler_params=pltpu.CompilerParams(collective_id=0, has_side_effects=True),
    )(
        layer_input.reshape(length, width),
        meta,
        query_weight,
        key_weight,
        value_weight,
        output_weight,
    )
    return (embedded.reshape(1, length, width), utility, expected.reshape(1))


def solution(mesh):
    in_specs = (
        P(("src", "cand"), None, None),
        P(("src", "cand"), None),
        P(("src", "cand")),
        P("src"),
        P("cand", None),
        P("cand", None),
        P("cand", None),
        P("cand", None),
    )
    out_specs = (P(("src", "cand"), None, None), P(("src", "cand"), None), P(("src", "cand")))
    return jax.shard_map(
        functools.partial(shards, dict(mesh.shape)),
        mesh=mesh,
        in_specs=in_specs,
        out_specs=out_specs,
        check_vma=False,
    )
```

```python
import functools
import math

import jax
import jax.numpy as jnp
from jax import lax
from jax.experimental import pallas as pl
from jax.experimental.pallas import tpu as pltpu
from jax.sharding import PartitionSpec as P

HEAD = 64


def block_utility(own_vectors, own_weight, far_vectors, far_weight):
    own_count, length, width = own_vectors.shape
    far_count = far_vectors.shape[0]
    similar = lax.dot_general(
        own_vectors.reshape(own_count * length, width),
        far_vectors.reshape(far_count * length, width),
        (((1,), (1,)), ((), ())),
        preferred_element_type=jnp.float32,
    )
    similar = similar.reshape(own_count, length, far_count, length)
    own_usable = own_weight > 0
    far_usable = far_weight > 0
    best_far = jnp.max(jnp.where(far_usable[None, None, :, :], similar, -4.0), axis=3)
    best_own = jnp.max(jnp.where(own_usable[:, :, None, None], similar, -4.0), axis=1)
    own_float = own_weight.astype(jnp.float32)
    far_float = far_weight.astype(jnp.float32)
    forward = jnp.einsum("il,ilj->ij", own_float, best_far, precision=lax.Precision.HIGHEST)
    forward = forward / jnp.sum(own_float, axis=1)[:, None]
    backward = jnp.einsum("jm,ijm->ij", far_float, best_own, precision=lax.Precision.HIGHEST)
    backward = backward / jnp.sum(far_float, axis=1)[None, :]
    return 0.5 * (forward + backward)


def gathered_shards(
    layer_input,
    token_ids,
    lengths,
    idf_table,
    query_weight,
    key_weight,
    value_weight,
    output_weight,
):
    local_cands, length, width = layer_input.shape
    cycle_size = lax.axis_size("cand")
    all_cands = local_cands * cycle_size
    head_size = HEAD
    head_count = width // head_size
    flat = layer_input.reshape(local_cands * length, width)
    pieces = (
        lax.all_gather(query_weight, "cand", axis=0, tiled=True),
        lax.all_gather(key_weight, "cand", axis=0, tiled=True),
        lax.all_gather(value_weight, "cand", axis=0, tiled=True),
    )
    columns = flat
    queries, key_rows, value_rows = tuple(
        (jnp.dot(columns, piece, preferred_element_type=jnp.float32) for piece in pieces)
    )
    queries = queries.astype(jnp.bfloat16).reshape(local_cands, length, head_count, head_size)
    key_rows = key_rows.astype(jnp.bfloat16).reshape(local_cands, length, head_count, head_size)
    value_rows = value_rows.astype(jnp.bfloat16).reshape(local_cands, length, head_count, head_size)
    positions = jnp.arange(length, dtype=jnp.int32)
    valid = positions[None, :] < lengths[:, None]
    scale = 1.0 / math.sqrt(head_size)
    scores = (
        jnp.einsum("clhe,cmhe->chlm", queries, key_rows, preferred_element_type=jnp.float32) * scale
    )
    scores = jnp.where(valid[:, None, None, :], scores, -1000000000.0)
    highest = jnp.max(scores, axis=-1, keepdims=True)
    expo = jnp.exp(scores - highest)
    probs = (expo / jnp.sum(expo, axis=-1, keepdims=True)).astype(jnp.bfloat16)
    context = jnp.einsum("chlm,cmhe->clhe", probs, value_rows, preferred_element_type=jnp.float32)
    context = context.astype(jnp.bfloat16).reshape(local_cands * length, width)
    columns = context
    mixed = jnp.dot(
        columns,
        lax.all_gather(output_weight, "cand", axis=0, tiled=True),
        preferred_element_type=jnp.float32,
    ) + flat.astype(jnp.float32)
    centred = mixed - jnp.mean(mixed, axis=-1, keepdims=True)
    squares = jnp.sum(centred * centred, axis=-1, keepdims=True)
    embedded = (
        (centred / jnp.sqrt(squares + 0.001))
        .astype(jnp.bfloat16)
        .reshape(local_cands, length, width)
    )
    token_weight = (jnp.take(idf_table, token_ids, axis=0) * valid.astype(jnp.float32)).astype(
        jnp.bfloat16
    )
    myself = lax.axis_index("cand")
    piece = (
        lax.all_gather(embedded, "cand", axis=0, tiled=True),
        lax.all_gather(token_weight, "cand", axis=0, tiled=True),
    )
    utility = block_utility(embedded, token_weight, piece[0], piece[1])
    blocks = utility.reshape(local_cands, cycle_size, local_cands)
    own_part = lax.dynamic_slice(blocks, (0, myself, 0), (local_cands, 1, local_cands))[:, 0, :]
    diagonal = jnp.diagonal(own_part)
    expected_utility = (jnp.sum(utility, axis=1) - diagonal) / (all_cands - 1)
    return (embedded, utility, expected_utility)


def remote(src_ref, dst_ref, send_sem, recv_sem, device):
    return pltpu.make_async_remote_copy(
        src_ref=src_ref,
        dst_ref=dst_ref,
        send_sem=send_sem,
        recv_sem=recv_sem,
        device_id=device,
        device_id_type=pl.DeviceIdType.MESH,
    )


def flipped(index, bits):
    result = index
    place = 1
    while place <= bits:
        if bits & place:
            digit = lax.rem(lax.div(index, place), 2)
            result = result + place - 2 * place * digit
        place *= 2
    return result


def kernel(
    count,
    x_hbm,
    ids_hbm,
    used,
    table_hbm,
    q_hbm,
    k_hbm,
    v_hbm,
    o_hbm,
    embedded_ref,
    utility_ref,
    expected_ref,
    stage,
    full,
    out_full,
    x_all,
    meta,
    context_out,
    context_full,
    vectors,
    ids,
    table,
    local_sem,
    send_sem,
    recv_sem,
):
    group, me = lax.axis_index("src"), lax.axis_index("cand")
    share = lax.rem(group, 4)
    sibling = (flipped(group, 1), me)
    mate = (flipped(group, 2), me)
    others = range(1, count)
    peer = [(group, flipped(me, bits)) for bits in range(count)]
    length, width = x_hbm.shape
    rows, columns = stage.shape[1], full.shape[2]
    quarter, middle = rows // 4, length // 2
    started = []

    def push(src_ref, dst_ref, device):
        number = len(started)
        copy = remote(src_ref, dst_ref, send_sem.at[number], recv_sem.at[number], device)
        copy.start()
        started.append(copy)
        return copy

    def column_block(index):
        return pl.ds(pl.multiple_of(index * columns, columns), columns)

    def row_block(index):
        return pl.ds(pl.multiple_of(index * rows, rows), rows)

    def row_share(index, which):
        return pl.ds(pl.multiple_of(index * rows + which * quarter, quarter), quarter)

    own_share = pl.ds(pl.multiple_of(share * quarter, quarter), quarter)
    mate_share = lax.rem(share + 2, 4)

    weights = (q_hbm, k_hbm, v_hbm)
    loads = [pltpu.make_async_copy(w, stage.at[t], local_sem.at[t]) for t, w in enumerate(weights)]
    loads += [
        pltpu.make_async_copy(o_hbm, out_full.at[row_block(me), :], local_sem.at[3]),
        pltpu.make_async_copy(x_hbm, x_all.at[0], local_sem.at[4]),
        pltpu.make_async_copy(ids_hbm, ids, local_sem.at[5]),
    ]
    loads += [
        pltpu.make_async_copy(
            w.at[:, column_block(me)], full.at[t, row_block(me), :], local_sem.at[6 + t]
        )
        for t, w in enumerate(weights)
    ]
    loads += [
        pltpu.make_async_copy(table_hbm, table, local_sem.at[9]),
    ]
    for load in loads:
        load.start()

    barrier = pltpu.get_barrier_semaphore()
    targets = [sibling, mate] + [peer[r] for r in others]
    for target in targets:
        pl.semaphore_signal(barrier, inc=1, device_id=target, device_id_type=pl.DeviceIdType.MESH)
    pl.semaphore_wait(barrier, len(targets))

    def exchange(held):
        part = [held.at[0, pl.ds(0, middle), :], held.at[0, pl.ds(middle, middle), :]]

        def slot(r, which):
            return held.at[r, pl.ds(which * middle, middle), :]

        first = {1: push(part[0], slot(1, 0), peer[1]), 2: push(part[1], slot(2, 1), peer[2])}
        second = {1: push(part[1], slot(1, 1), peer[1]), 2: push(part[0], slot(2, 0), peer[2])}

        def relay():
            first[1].wait_recv()
            near = push(slot(1, 0), slot(3, 0), peer[2])
            first[2].wait_recv()
            return (near, push(slot(2, 1), slot(3, 1), peer[1]))

        return second, relay

    for t in range(3):
        loads[t].wait()
    w_copies = {}
    for r in others:
        w_copies[r] = push(
            stage.at[:, own_share, column_block(peer[r][1])],
            full.at[:, row_share(me, share), :],
            peer[r],
        )
    for load in loads[3:6]:
        load.wait()
    o_copies = {
        r: push(out_full.at[row_share(me, share), :], out_full.at[row_share(me, share), :], peer[r])
        for r in others
    }
    x_second, x_relay = exchange(x_all)
    for load in loads[6:]:
        load.wait()

    position = lax.broadcasted_iota(jnp.int32, (1, length), 1)

    def look_up(at, weights_row):
        return jnp.where(position == at, table[ids[0, at]], weights_row)

    valid_row = (position < used[0]).astype(jnp.float32)
    weights_row = lax.fori_loop(0, length, look_up, jnp.zeros((1, length), jnp.float32), unroll=8)
    weights_row = (weights_row * valid_row).astype(jnp.bfloat16).astype(jnp.float32)
    meta[0] = jnp.concatenate([weights_row, jnp.broadcast_to(valid_row, (7, length))], axis=0)
    m_copies = {r: push(meta.at[0], meta.at[r], peer[r]) for r in others}

    def spread(copy, landed):
        copy.wait_recv()
        return (push(landed, landed, mate), push(landed, landed, sibling))

    def hand_over(copy, landed):
        copy.wait_recv()
        return push(landed, landed, sibling)

    def full_share(r, which):
        return full.at[:, row_share(peer[r][1], which), :]

    def out_share(r, which):
        return out_full.at[row_share(peer[r][1], which), :]

    w_spread = {r: spread(w_copies[r], full_share(r, share)) for r in others}
    o_spread = {}
    o_hand = {}
    for r in others:
        o_spread[r] = spread(o_copies[r], out_share(r, share))
    w_hand = {r: hand_over(w_spread[r][0], full_share(r, mate_share)) for r in others}
    x_far = x_relay()
    for r in others:
        w_spread[r][1].wait_recv()
        w_hand[r].wait_recv()

    lane = lax.broadcasted_iota(jnp.int32, (1, 2 * HEAD), 1)
    scale = 1.0 / math.sqrt(HEAD)
    first = (lane < HEAD).astype(jnp.float32)
    keep = [(first * scale).astype(jnp.bfloat16), ((1.0 - first) * scale).astype(jnp.bfloat16)]

    def context_of(r):
        rows_in = x_all[r]
        queries, key_rows, value_rows = tuple(
            jnp.dot(rows_in, full[t], preferred_element_type=jnp.float32).astype(jnp.bfloat16)
            for t in range(3)
        )
        valid = meta[r, 1:2, :] > 0.0
        pieces = []
        for start in range(0, columns, 2 * HEAD):
            span = slice(start, start + 2 * HEAD)
            q_pair, k_pair, v_pair = queries[:, span], key_rows[:, span], value_rows[:, span]
            stacked = jnp.concatenate([q_pair * keep[0], q_pair * keep[1]], axis=0)
            scores = lax.dot_general(
                stacked, k_pair, (((1,), (1,)), ((), ())), preferred_element_type=jnp.float32
            )
            scores = jnp.where(valid, scores, -1000000000.0)
            expo = jnp.exp(scores - jnp.max(scores, axis=-1, keepdims=True))
            total = jnp.sum(expo, axis=-1, keepdims=True)
            summed = jnp.dot(
                expo.astype(jnp.bfloat16), v_pair, preferred_element_type=jnp.float32
            )
            summed = summed / total
            pieces.append(jnp.where(lane < HEAD, summed[:length], summed[length:]))
        return jnp.concatenate(pieces, axis=1).astype(jnp.bfloat16)

    context_full[:, column_block(me)] = context_of(0)
    c_copies = []
    for r in others:
        m_copies[r].wait_recv()
        for copy in ((x_second[r],) if r < 3 else x_far):
            copy.wait_recv()
        context_out[r] = context_of(r)
        c_copies.append(push(context_out.at[r], context_full.at[:, column_block(me)], peer[r]))
        if r == 2:
            for q in others:
                o_hand[q] = hand_over(o_spread[q][0], out_share(q, mate_share))
    for r in others:
        o_spread[r][1].wait_recv()
        o_hand[r].wait_recv()
    for copy in c_copies:
        copy.wait_recv()

    mixed = jnp.dot(context_full[...], out_full[...], preferred_element_type=jnp.float32)
    mixed = mixed + x_all[0].astype(jnp.float32)
    centred = mixed - jnp.mean(mixed, axis=-1, keepdims=True)
    squares = jnp.sum(centred * centred, axis=-1, keepdims=True)
    own = (centred / jnp.sqrt(squares + 0.001)).astype(jnp.bfloat16)
    vectors[0] = own
    e_second, e_relay = exchange(vectors)
    embedded_ref[...] = own

    own_weight = meta[0, 0:1, :]
    own_column = jnp.broadcast_to(own_weight, (length, length)).T
    own_total = jnp.sum(own_weight, axis=1, keepdims=True)
    slot = lax.broadcasted_iota(jnp.int32, utility_ref.shape, 1)

    def pair_of(r):
        far_weight = meta[r, 0:1, :]
        similar = lax.dot_general(
            own, vectors[r], (((1,), (1,)), ((), ())), preferred_element_type=jnp.float32
        )
        best_far = jnp.max(jnp.where(far_weight > 0, similar, -4.0), axis=1, keepdims=True)
        best_own = jnp.max(jnp.where(own_column > 0, similar, -4.0), axis=0, keepdims=True)
        forward = jnp.sum(own_column[:, 0:1] * best_far, axis=0, keepdims=True) / own_total
        backward = jnp.sum(far_weight * best_own, axis=1, keepdims=True) / jnp.sum(
            far_weight, axis=1, keepdims=True
        )
        return 0.5 * (forward + backward)

    diagonal = pair_of(0)
    e_far = e_relay()
    utility = jnp.where(slot == me, diagonal, 0.0)
    everything = diagonal
    for r in others:
        for copy in ((e_second[r],) if r < 3 else e_far):
            copy.wait_recv()
        pair = pair_of(r)
        utility = jnp.where(slot == peer[r][1], pair, utility)
        everything = everything + pair
    utility_ref[...] = utility
    expected_ref[...] = (everything - diagonal) / (count - 1)

    for copy in started:
        copy.wait_send()


def shards(
    sizes,
    layer_input,
    token_ids,
    lengths,
    idf_table,
    query_weight,
    key_weight,
    value_weight,
    output_weight,
):
    local_cands, length, width = layer_input.shape
    count = sizes["cand"]
    rows = query_weight.shape[0]
    columns = width // count
    if (
        local_cands != 1
        or count != 4
        or sizes["src"] % 4
        or columns % (2 * HEAD)
        or rows % 64
        or length != 128
    ):
        return gathered_shards(
            layer_input,
            token_ids,
            lengths,
            idf_table,
            query_weight,
            key_weight,
            value_weight,
            output_weight,
        )
    anywhere = pl.BlockSpec(memory_space=pl.ANY)
    in_vmem = pl.BlockSpec(memory_space=pltpu.VMEM)
    copies = pltpu.SemaphoreType.DMA((42,))
    embedded, utility, expected = pl.pallas_call(
        functools.partial(kernel, count),
        out_shape=(
            pltpu.VMEM((length, width), jnp.bfloat16),
            pltpu.VMEM((1, count), jnp.float32),
            pltpu.VMEM((1, 1), jnp.float32),
        ),
        in_specs=[anywhere] * 2 + [pl.BlockSpec(memory_space=pltpu.SMEM)] + [anywhere] * 5,
        out_specs=(in_vmem, in_vmem, in_vmem),
        scratch_shapes=[
            pltpu.VMEM((3, rows, width), jnp.bfloat16),
            pltpu.VMEM((3, rows * count, columns), jnp.bfloat16),
            pltpu.VMEM((rows * count, width), jnp.bfloat16),
            pltpu.VMEM((count, length, width), jnp.bfloat16),
            pltpu.VMEM((count, 8, length), jnp.float32),
            pltpu.VMEM((count, length, columns), jnp.bfloat16),
            pltpu.VMEM((length, width), jnp.bfloat16),
            pltpu.VMEM((count, length, width), jnp.bfloat16),
            pltpu.SMEM((1, length), jnp.int32),
            pltpu.SMEM(idf_table.shape, jnp.float32),
            pltpu.SemaphoreType.DMA((10,)),
            copies,
            copies,
        ],
        compiler_params=pltpu.CompilerParams(collective_id=0, has_side_effects=True),
    )(
        layer_input.reshape(length, width),
        token_ids,
        lengths,
        idf_table,
        query_weight,
        key_weight,
        value_weight,
        output_weight,
    )
    return (embedded.reshape(1, length, width), utility, expected.reshape(1))


def solution(mesh):
    in_specs = (
        P(("src", "cand"), None, None),
        P(("src", "cand"), None),
        P(("src", "cand")),
        P("src"),
        P("cand", None),
        P("cand", None),
        P("cand", None),
        P("cand", None),
    )
    out_specs = (P(("src", "cand"), None, None), P(("src", "cand"), None), P(("src", "cand")))
    return jax.shard_map(
        functools.partial(shards, dict(mesh.shape)),
        mesh=mesh,
        in_specs=in_specs,
        out_specs=out_specs,
        check_vma=False,
    )
```
